128 devices in a mesh: rep: 1, r: 4 (over x), s: 32 (over y, z, core).
Axes of the slice: x: 4, y: 4, z: 4, core: 2. Of those that a mesh axis runs over, the one named last changes fastest.
Arguments:
- x: bfloat16 [128, 2048, 1024], P(('rep', 'r', 's'))
- dy: bfloat16 [128, 2048, 1024], P(('rep', 'r', 's'))
- w_gate: bfloat16 [2, 1024, 3584], P(None, 's')
- w_up: bfloat16 [2, 1024, 3584], P(None, 's')
- w_down: bfloat16 [2, 3584, 1024], P(None, 's')
- m_w_gate: float32 [2, 1024, 3584], P(None, 's')
- m_w_up: float32 [2, 1024, 3584], P(None, 's')
- m_w_down: float32 [2, 3584, 1024], P(None, 's')
- v_w_gate: float32 [2, 1024, 3584], P(None, 's')
- v_w_up: float32 [2, 1024, 3584], P(None, 's')
- v_w_down: float32 [2, 3584, 1024], P(None, 's')
Outputs:
- output 1: bfloat16 [2, 1024, 3584], P('rep', 's')
- output 2: bfloat16 [2, 1024, 3584], P('rep', 's')
- output 3: bfloat16 [2, 3584, 1024], P('rep', 's')
- output 4: float32 [2, 1024, 3584], P('rep', 's')
- output 5: float32 [2, 1024, 3584], P('rep', 's')
- output 6: float32 [2, 3584, 1024], P('rep', 's')
- output 7: float32 [2, 1024, 3584], P('rep', 's')
- output 8: float32 [2, 1024, 3584], P('rep', 's')
- output 9: float32 [2, 3584, 1024], P('rep', 's')
All inputs are finite; a program needn't handle non-finite values.
Results may differ from the reference program's by a relative error of at most 0.022.
Values are sent between devices in bfloat16 or wider.
A program may use at most 1.5 GiB of HBM per device.

```python
import jax
import jax.numpy as jnp
from jax import lax

SEQUENCES = 128
TOKENS = 2048
D = 1024
FF = 3584
LAYERS = 2
NAMES = ("w_gate", "w_up", "w_down")
SHAPES = {"w_gate": (LAYERS, D, FF), "w_up": (LAYERS, D, FF), "w_down": (LAYERS, FF, D)}


def bump(key, n, height):
    away = (jnp.arange(n, dtype=jnp.int32) - jax.random.randint(key, (), 0, n, jnp.int32)) % n
    return jnp.where(away < n // 8, height, 1.0)


def together(key, own, strength):
    shared = jax.random.normal(key, own.shape[1:], jnp.float32)
    return (own + strength * shared) * lax.rsqrt(1 + strength * strength)


def setup_inputs(seed: int = 0, part: int = 0) -> dict:
    kx, kdy, ka, kb, kz, kf, kh, kl, *keys = jax.random.split(jax.random.key(seed), 8 + 3 * len(NAMES))
    kx, kdy, ka, kb = (jax.random.fold_in(k, part) for k in (kx, kdy, ka, kb))
    kw, km, kv = (keys[i::3] for i in range(3))
    shape = (SEQUENCES, TOKENS, D)
    much_x, much_dy = jax.random.uniform(kz, (2,), jnp.float32, 0.0, 1.0)
    loud = 2.0 ** jax.random.uniform(jax.random.fold_in(kz, 1), (), jnp.float32, -1.0, 2.0)
    layers = 2.0 ** jax.random.uniform(kl, (LAYERS, 1, 1), jnp.float32, -1.0, 1.0)
    x = together(ka, jax.random.normal(kx, shape, jnp.float32), much_x) * bump(kf, D, 4.0)
    dy = together(kb, jax.random.normal(kdy, shape, jnp.float32), much_dy)
    drawn = {"x": x.astype(jnp.bfloat16), "dy": (loud * dy * (SEQUENCES * TOKENS) ** -0.5).astype(jnp.bfloat16)}
    for key, name in zip(kw, NAMES, strict=True):
        w = jax.random.normal(key, SHAPES[name], jnp.float32) * SHAPES[name][1] ** -0.5
        drawn[name] = (w * {"w_gate": 1.0, "w_up": bump(kh, FF, 4.0), "w_down": layers}[name]).astype(jnp.bfloat16)
    for key, name in zip(km, NAMES, strict=True):
        drawn[f"m_{name}"] = 0.1 * jax.random.normal(key, SHAPES[name], jnp.float32)
    for key, name in zip(kv, NAMES, strict=True):
        drawn[f"v_{name}"] = loud * loud * jax.random.uniform(key, SHAPES[name], jnp.float32, 0.05, 0.15)
    return drawn


def matmul(a, w):
    return jnp.dot(a, w, preferred_element_type=jnp.float32).astype(jnp.bfloat16)


def normed(h):
    wide = h.astype(jnp.float32)
    scale = lax.rsqrt(jnp.mean(wide**2, -1, keepdims=True) + 1e-6)
    return (wide * scale).astype(jnp.bfloat16)


def layer(h, w):
    a = normed(h)
    gate = jnp.dot(a, w["w_gate"], preferred_element_type=jnp.float32)
    up = jnp.dot(a, w["w_up"], preferred_element_type=jnp.float32)
    return h + matmul((jax.nn.silu(gate) * up).astype(jnp.bfloat16), w["w_down"])


def adamw(w, m, v, g):
    m = 0.9 * m + 0.1 * g
    v = 0.95 * v + 0.05 * g * g
    step = m * lax.rsqrt(v + 1e-8) + 0.1 * w
    return (w - 0.02 * step).astype(jnp.bfloat16), m, v


def stack(weights, h):
    return lax.scan(lambda h, w: (layer(h, w), None), h, weights)[0]


def reference(x, dy, w_gate, w_up, w_down, m_w_gate, m_w_up, m_w_down, v_w_gate, v_w_up, v_w_down):
    weights = dict(zip(NAMES, (w_gate, w_up, w_down), strict=True))

    def take(so_far, sequence):
        h, by_y = sequence
        _, back = jax.vjp(lambda w: stack(w, h), weights)
        return jax.tree.map(lambda total, term: total + term.astype(jnp.float32), so_far, back(by_y)[0]), None

    none_yet = {name: jnp.zeros(w.shape, jnp.float32) for name, w in weights.items()}
    by_weights, _ = lax.scan(take, none_yet, (x, dy))
    gradients = [by_weights[name].astype(jnp.bfloat16).astype(jnp.float32) for name in NAMES]
    new = [
        adamw(w.astype(jnp.float32), m, v, g)
        for w, m, v, g in zip((w_gate, w_up, w_down), (m_w_gate, m_w_up, m_w_down), (v_w_gate, v_w_up, v_w_down), gradients, strict=True)
    ]
    return tuple(one[which] for which in range(3) for one in new)
```

```python
import functools

import jax
import jax.numpy as jnp
from jax import lax
from jax.experimental import pallas as pl
from jax.experimental.pallas import tpu as pltpu
from jax.sharding import PartitionSpec as P

BF, F32 = jnp.bfloat16, jnp.float32
MESH = pl.DeviceIdType.MESH
ANY = pl.BlockSpec(memory_space=pl.ANY)
TT, UU, VV = 0, 1, 2


def place():
    s = lax.axis_index("s")
    return lax.axis_index("r"), s // 8, (s // 2) % 4, s % 2


def at_s(y, z, c):
    return {"s": (y * 4 + z) * 2 + c}


def step_to(k, d):
    return lax.rem(k + d + 4, 4)


def mate(order, which, d):
    _, y, z, c = place()
    along_y = (order == 0) == (which == 0)
    return at_s(step_to(y, d), z, c) if along_y else at_s(y, step_to(z, d), c)


def partner():
    _, y, z, c = place()
    return at_s(y, z, 1 - c)


def remote(src, dst, send, recv, to):
    return pltpu.make_async_remote_copy(src_ref=src, dst_ref=dst, send_sem=send, recv_sem=recv, device_id=to, device_id_type=MESH)


class Gather:
    far = False

    def __init__(self, order, shard):
        self.order = order
        rows, cols = shard.shape
        self.rows, self.cols = rows, cols
        self.inputs = [shard]
        self.outs = [jax.ShapeDtypeStruct((4, 4, 2, rows, cols), BF)]
        self.out_specs = [ANY]
        self.scratch = [pltpu.VMEM((rows, cols), BF), pltpu.SemaphoreType.DMA((15,)), pltpu.SemaphoreType.DMA((15,)), pltpu.SemaphoreType.DMA((2,))]

    def events(self, ins, outs, scratch):
        (own,), (full,) = ins, outs
        hold, ss, rs, local = scratch
        o, half = self.order, self.cols // 2
        _, y, z, c = place()
        f, g = (y, z) if o == 0 else (z, y)

        def block(fk, gk, core):
            return full.at[fk, gk, core] if o == 0 else full.at[gk, fk, core]

        def column(gk, core):
            return full.at[:, gk, core] if o == 0 else full.at[gk, :, core]

        lo, hi = pl.ds(0, half), pl.ds(half, half)
        fp, fm, f2 = step_to(f, 1), step_to(f, -1), step_to(f, 2)
        gp, gm, g2 = step_to(g, 1), step_to(g, -1), step_to(g, 2)
        me = block(f, g, c)

        def cols_of(gk, part):
            return full.at[:, gk, c, :, part] if o == 0 else full.at[gk, :, c, :, part]

        def part_of(fk, part):
            return full.at[fk, g, c, :, part] if o == 0 else full.at[g, fk, c, :, part]

        up1, dn1 = mate(o, 0, 1), mate(o, 0, -1)
        up2, dn2 = mate(o, 1, 1), mate(o, 1, -1)
        p = partner()
        table = [
            (own, me, block(fm, g, c), up1),
            (own, me, block(fp, g, c), dn1),
            (part_of(fm, lo), part_of(fm, lo), part_of(f2, lo), up1),
            (part_of(fp, hi), part_of(fp, hi), part_of(f2, hi), dn1),
            (column(g, c), column(g, c), column(gm, c), up2),
            (column(g, c), column(g, c), column(gp, c), dn2),
            (cols_of(gm, lo), cols_of(gm, lo), cols_of(g2, lo), up2),
            (cols_of(gp, hi), cols_of(gp, hi), cols_of(g2, hi), dn2),
            (own, me, block(f, g, 1 - c), p),
            (block(fm, g, c), block(fm, g, c), block(fm, g, 1 - c), p),
            (block(fp, g, c), block(fp, g, c), block(fp, g, 1 - c), p),
            (block(f2, g, c), block(f2, g, c), block(f2, g, 1 - c), p),
            (column(gm, c), column(gm, c), column(gm, 1 - c), p),
            (column(gp, c), column(gp, c), column(gp, 1 - c), p),
            (column(g2, c), column(g2, c), column(g2, 1 - c), p),
        ]

        def start(*numbers):
            for n in numbers:
                src, dst, _, to = table[n]
                remote(src, dst, ss.at[n], rs.at[n], to).start()

        def arrived(*numbers):
            for n in numbers:
                _, _, here, to = table[n]
                remote(here, here, ss.at[n], rs.at[n], to).wait_recv()

        def e0():
            start(0, 1, 8)
            pltpu.make_async_copy(own, hold, local.at[0]).start()

        def e1():
            pltpu.make_async_copy(own, hold, local.at[0]).wait()
            pltpu.make_async_copy(hold, me, local.at[1]).start()
            arrived(0, 1)
            start(2, 3, 9, 10)

        def e2():
            pltpu.make_async_copy(hold, me, local.at[1]).wait()
            arrived(2, 3)
            start(4, 5, 11)

        def e3():
            arrived(4, 5)
            start(6, 7, 12, 13)

        def e4():
            arrived(6, 7)
            start(14)

        def e5():
            arrived(*range(8, 15))
            for n in range(15):
                src, dst, _, to = table[n]
                remote(src, dst, ss.at[n], rs.at[n], to).wait_send()

        return [e0, e1, e2, e3, e4, e5]


def added(*refs_at):
    total = refs_at[0].astype(F32)
    for r in refs_at[1:]:
        total = total + r.astype(F32)
    return total.astype(BF)


class Ring:
    def __init__(self, slot, n, got, ss, rs, k, up, down):
        self.slot, self.n, self.got, self.ss, self.rs = slot, n, got, ss, rs
        self.k, self.up, self.down = k, up, down

    def copy(self, kind, d):
        k, a = self.k, d
        if kind == TT:
            src = self.slot(a, step_to(k, 2))
        elif kind == UU:
            src = self.slot(1 - a, step_to(k, 1 - 2 * d))
        else:
            src = self.slot(a, step_to(k, 1 - 2 * d))
        return remote(src, self.got.at[kind, d], self.ss.at[kind, d], self.rs.at[kind, d], self.down if d else self.up)

    def first(self):
        for d in (0, 1):
            self.copy(TT, d).start()
        for d in (0, 1):
            self.copy(UU, d).start()

    def second_add(self):
        for d in (0, 1):
            self.copy(TT, d).wait_recv()
        for d in (0, 1):
            ref = self.slot(d, step_to(self.k, 1 - 2 * d))
            for i in range(self.n):
                ref[i] = added(ref[i], self.got[TT, d, i])

    def second_send(self):
        for d in (0, 1):
            self.copy(VV, d).start()

    def last(self, out):
        for kind in (UU, VV):
            for d in (0, 1):
                self.copy(kind, d).wait_recv()
        for a in (0, 1):
            ref = self.slot(a, self.k)
            for i in range(self.n):
                out(a, i, added(ref[i], self.got[VV, a, i], self.got[UU, 1 - a, i]))

    def drain(self):
        for kind in (TT, UU, VV):
            for d in (0, 1):
                self.copy(kind, d).wait_send()


class SumA:
    far = False

    def __init__(self, grad):
        rows, cols = grad.shape
        self.R, self.C = rows // 32, cols // 4
        R, C = self.R, self.C
        self.inputs = [grad.reshape(4, 4, 2, R, cols)]
        self.outs = [jax.ShapeDtypeStruct((2, 2, 4, R, C), BF)]
        self.out_specs = [ANY]
        D = pltpu.SemaphoreType.DMA
        self.scratch = [pltpu.VMEM((4, 4, 4, R, C), BF), pltpu.VMEM((4, 4, 4, R, C), BF), pltpu.VMEM((2, 3, 2, 4, R, C), BF), pltpu.VMEM((2, 2, 4, R, C), BF)]
        self.scratch += [D((4,)), D((4,)), D((4,)), D((2, 3, 2)), D((2, 3, 2)), D]

    def events(self, ins, outs, scratch):
        (g,), (out,) = ins, outs
        H, other, got, F, ls, ds, dr, ss, rs, os = scratch
        C = self.C
        _, y, z, c = place()

        def load(q):
            return pltpu.make_async_copy(g.at[:, :, c, :, pl.ds(q * C, C)], H.at[q], ls.at[q])

        def cross(q):
            return remote(g.at[:, :, 1 - c, :, pl.ds(q * C, C)], other.at[q], ds.at[q], dr.at[q], partner())

        def slot(o):
            return lambda ab, k: H.at[2 * o + ab, k] if o == 0 else H.at[2 * o + ab, :, k]

        rings = [Ring(slot(o), 4, got.at[o], ss.at[o], rs.at[o], (y, z)[o], mate(o, 0, 1), mate(o, 0, -1)) for o in (0, 1)]

        def e0():
            for q in range(4):
                cross(q).start()
                load(q).start()

        def e1():
            for q in range(4):
                load(q).wait()
                cross(q).wait_recv()

                def body(i, _):
                    a, b = i // 4, i % 4
                    H[q, a, b] = added(H[q, a, b], other[q, a, b])
                    return 0

                lax.fori_loop(0, 16, body, 0)

        def e2():
            for r in rings:
                r.first()

        def e3():
            for r in rings:
                r.second_add()

        def e4():
            for r in rings:
                r.second_send()

        def e5():
            for o, r in enumerate(rings):

                def put(a, i, value, o=o):
                    F[o, a, i] = value

                r.last(put)

        def e6():
            pltpu.make_async_copy(F, out, os).start()
            for r in rings:
                r.drain()
            for q in range(4):
                cross(q).wait_send()
            pltpu.make_async_copy(F, out, os).wait()

        return [e0, e1, e2, e3, e4, e5, e6]


class SumB:
    far = True

    def __init__(self, part):
        _, _, _, R, C = part.shape
        self.R, self.C = R, C
        self.inputs = [part]
        self.outs = [jax.ShapeDtypeStruct((R, 4 * C), BF)]
        self.out_specs = [ANY]
        D = pltpu.SemaphoreType.DMA
        self.scratch = [pltpu.VMEM((2, 2, 4, R, C), BF), pltpu.VMEM((2, 3, 2, 1, R, C), BF), pltpu.VMEM((4, 4, R, C), BF), pltpu.VMEM((R, 4 * C), BF)]
        self.scratch += [D, D((2, 3, 2)), D((2, 3, 2)), D((3,)), D((3,)), D]

    def events(self, ins, outs, scratch):
        (part,), (out,) = ins, outs
        F, got, X, done, ls, ss, rs, xs, xr, os = scratch
        C = self.C
        x, y, z, c = place()

        def slot(o):
            return lambda ab, k: F.at[o, ab, pl.ds(k, 1)]

        rings = [Ring(slot(o), 1, got.at[o], ss.at[o], rs.at[o], (z, y)[o], mate(o, 1, 1), mate(o, 1, -1)) for o in (0, 1)]

        def over(d):
            return remote(X.at[x], X.at[x], xs.at[d - 1], xr.at[d - 1], {"r": step_to(x, d)})

        def came(d):
            src = X.at[step_to(x, -d)]
            return remote(src, src, xs.at[d - 1], xr.at[d - 1], {"r": step_to(x, d)})

        def e0():
            pltpu.make_async_copy(part, F, ls).start()
            pltpu.make_async_copy(part, F, ls).wait()
            for r in rings:
                r.first()

        def e1():
            for r in rings:
                r.second_add()

        def e2():
            for r in rings:
                r.second_send()

        def e3():
            for o, r in enumerate(rings):

                def put(a, i, value, o=o):
                    X[x, 2 * o + a] = value

                r.last(put)

        def e4():
            for d in (1, 3, 2):
                over(d).start()

        def e5():
            for d in (1, 3, 2):
                came(d).wait_recv()
            for q in range(4):
                done[:, q * C : (q + 1) * C] = added(*(X[i, q] for i in range(4)))

        def e6():
            pltpu.make_async_copy(done, out, os).start()
            for r in rings:
                r.drain()
            for d in (1, 3, 2):
                over(d).wait_send()
            pltpu.make_async_copy(done, out, os).wait()

        return [e0, e1, e2, e3, e4, e5, e6]


def run(name, number, steps, arrays, specs, outs, out_specs, compute, jobs=(), when=None, flops=0):
    n_in, n_out = len(arrays), len(outs)
    job_in = [a for j in jobs for a in j.inputs]
    job_out = [a for j in jobs for a in j.outs]

    def body(*refs):
        ins, rest = refs[:n_in], refs[n_in:]
        jin, rest = rest[: len(job_in)], rest[len(job_in) :]
        mouts, rest = rest[:n_out], rest[n_out:]
        jout, scratch = rest[: len(job_out)], rest[len(job_out) :]
        t = pl.program_id(0)
        lists = []
        for j in jobs:
            a, jin = jin[: len(j.inputs)], jin[len(j.inputs) :]
            b, jout = jout[: len(j.outs)], jout[len(j.outs) :]
            c, scratch = scratch[: len(j.scratch)], scratch[len(j.scratch) :]
            lists.append(j.events(a, b, c))
        if jobs:

            @pl.when(t == 0)
            def _():
                barrier = pltpu.get_barrier_semaphore()
                them = [mate(0, w, d) for w in (0, 1) for d in (1, -1)] + [partner()]
                if any(j.far for j in jobs):
                    x = lax.axis_index("r")
                    them += [{"r": step_to(x, d)} for d in (1, 2, 3)]
                for device in them:
                    pl.semaphore_signal(barrier, inc=1, device_id=device, device_id_type=MESH)
                pl.semaphore_wait(barrier, len(them))

        table = {}
        for j, events in enumerate(lists):
            for i, e in enumerate(events):
                at = when[j][i] if when and i < len(when[j]) else steps
                table.setdefault(min(at, steps), []).append((i, j, e))
        for at in sorted(table):
            if at < steps:

                @pl.when(t == at)
                def _(at=at):
                    for _, _, e in sorted(table[at], key=lambda v: v[:2]):
                        e()

        if compute is not None:
            compute(t, ins, mouts)
        if steps in table:

            @pl.when(t == steps - 1)
            def _():
                for _, _, e in sorted(table[steps], key=lambda v: v[:2]):
                    e()

    got = pl.pallas_call(
        body,
        name=name,
        grid=(steps,),
        out_shape=list(outs) + job_out,
        in_specs=list(specs) + [ANY] * len(job_in),
        out_specs=list(out_specs) + [s for j in jobs for s in j.out_specs],
        scratch_shapes=[s for j in jobs for s in j.scratch],
        compiler_params=pltpu.CompilerParams(
            dimension_semantics=("arbitrary",),
            vmem_limit_bytes=66_000_000,
            **(dict(collective_id=number, has_side_effects=True) if jobs else {}),
        ),
        cost_estimate=pl.CostEstimate(flops=flops, bytes_accessed=50_000_000, transcendentals=0),
    )(*arrays, *job_in)
    return list(got)


def fixed(shape):
    return pl.BlockSpec(shape, lambda t: (0,) * len(shape), pipeline_mode=pl.Buffered(1))


def across(rows, cols):
    return pl.BlockSpec((rows, cols), lambda t: (0, t))


def down_by(rows, cols):
    return pl.BlockSpec((rows, cols), lambda t: (t, 0))


def nn(a, b):
    return jnp.dot(a, b, preferred_element_type=F32)


def nt(a, b):
    return lax.dot_general(a, b, (((1,), (1,)), ((), ())), preferred_element_type=F32)


def tn(a, b):
    return lax.dot_general(a, b, (((0,), (0,)), ((), ())), preferred_element_type=F32)


def shape(*dims, dtype=BF):
    return jax.ShapeDtypeStruct(dims, dtype)


ROWS = 512


def by_rows(total, fn):
    def body(i, _):
        fn(pl.ds(pl.multiple_of(i * ROWS, ROWS), ROWS))
        return 0

    lax.fori_loop(0, total // ROWS, body, 0)


def glu(t, ins, outs):
    a, wg, wu = ins
    gate_ref, up_ref, hid_ref = outs

    def part(rows):
        gate, up = nn(a[rows, :], wg[...]), nn(a[rows, :], wu[...])
        gate_ref[rows, :] = gate
        up_ref[rows, :] = up
        hid_ref[rows, :] = (gate * jax.nn.sigmoid(gate) * up).astype(BF)

    by_rows(a.shape[0], part)


def glu_back(by_hid, gate, up):
    by_hid = by_hid.astype(BF).astype(F32)
    sig = jax.nn.sigmoid(gate)
    act = gate * sig
    return (act * up).astype(BF), (by_hid * up * (sig + act * (1.0 - sig))).astype(BF), (by_hid * act).astype(BF)


def both_ways(t, ins, outs):
    a, dy, wg, wu, wd = ins
    hid_ref, dg_ref, du_ref = outs

    def part(rows):
        gate, up = nn(a[rows, :], wg[...]), nn(a[rows, :], wu[...])
        hid_ref[rows, :], dg_ref[rows, :], du_ref[rows, :] = glu_back(nt(dy[rows, :], wd[...]), gate, up)

    by_rows(a.shape[0], part)


def back(t, ins, outs):
    dy, wd, gate, up = ins
    dg_ref, du_ref = outs

    def part(rows):
        _, dg_ref[rows, :], du_ref[rows, :] = glu_back(nt(dy[rows, :], wd[...]), gate[rows, :], up[rows, :])

    by_rows(dy.shape[0], part)


def lower(t, ins, outs):
    hid, wd, h = ins
    outs[0][...] = h[...] + nn(hid[...], wd[...]).astype(BF)


def grad_two(t, ins, outs):
    at, dg, du = ins
    outs[0][...] = nn(at[...], dg[...]).astype(BF)
    outs[1][...] = nn(at[...], du[...]).astype(BF)


def grad_down(t, ins, outs):
    hid, dy = ins
    outs[0][...] = tn(hid[...], dy[...]).astype(BF)


def grad_a(t, ins, outs):
    dg, du, wg, wu = ins
    outs[0][...] = nt(dg[...], wg[...]).astype(BF) + nt(du[...], wu[...]).astype(BF)


def normed(h):
    wide = h.astype(F32)
    scale = lax.rsqrt(jnp.mean(wide**2, -1, keepdims=True) + 1e-6)
    return (wide * scale).astype(BF)


def adamw(w, m, v, g):
    m = 0.9 * m + 0.1 * g
    v = 0.95 * v + 0.05 * g * g
    step = m * lax.rsqrt(v + 1e-8) + 0.1 * w
    return (w - 0.02 * step).astype(BF), m, v


def solution(mesh):
    def step(x, dy, *arrays):
        (wg, wu, wd), m, v = (arrays[i : i + 3] for i in (0, 3, 6))
        x, dy = x[0], dy[0]
        N, D = x.shape
        FF = wg.shape[2]
        B, TB = 256, 256
        T, TN = FF // B, N // TB
        one = 2 * N * D * FF
        flat = lambda w: w.reshape(-1, w.shape[-1])
        tok, wide, ffd = (N, D), shape(N, FF), shape(FF, D)

        wg1, wu1 = map(flat, run("fetch_0", 1, 1, [], [], [], [], None, [Gather(0, wg[0]), Gather(1, wu[0])], flops=one))
        a1 = normed(x)
        gate1, up1, hid1, wd1, wg2 = run(
            "glu_0", 2, T, [a1, wg1, wu1], [fixed(tok), across(D, B), across(D, B)],
            [shape(N, FF, dtype=F32), shape(N, FF, dtype=F32), wide], [across(N, B)] * 3, glu,
            [Gather(0, wd[0]), Gather(1, wg[1])], [[0, 2, 4, 8, 12], [0, 2, 4, 8, 12]], 2 * one,
        )
        wd1, wg2 = flat(wd1), flat(wg2)
        h1, wu2, wd2 = run(
            "lower_0", 3, TN, [hid1, wd1, x], [down_by(TB, FF), fixed((FF, D)), down_by(TB, D)],
            [shape(N, D)], [down_by(TB, D)], lower,
            [Gather(0, wu[1]), Gather(1, wd[1])], [[0, 2, 4], [0, 2, 4]], one,
        )
        wu2, wd2 = flat(wu2), flat(wd2)
        a2, back_norm = jax.vjp(normed, h1)
        hid2, dg2, du2 = run(
            "both_1", 0, T, [a2, dy, wg2, wu2, wd2], [fixed(tok), fixed(tok), across(D, B), across(D, B), down_by(B, D)],
            [wide] * 3, [across(N, B)] * 3, both_ways, flops=3 * one,
        )
        (gd2,) = run("grad_down_1", 0, T, [hid2, dy], [across(N, B), fixed(tok)], [ffd], [down_by(B, D)], grad_down, flops=one)
        gg2, gu2, fd2 = run(
            "grad_two_1", 4, T, [a2.T, dg2, du2], [fixed((D, N)), across(N, B), across(N, B)],
            [shape(D, FF)] * 2, [across(D, B)] * 2, grad_two, [SumA(gd2)], [[0, 3, 4, 9, 10]], 2 * one,
        )
        by_a, fg2, sd2 = run(
            "grad_a_1", 5, TN, [dg2, du2, wg2, wu2], [down_by(TB, FF)] * 2 + [fixed((D, FF))] * 2,
            [shape(N, D)], [down_by(TB, D)], grad_a, [SumA(gg2), SumB(fd2)], [[0, 2, 3, 6, 7], [0, 1, 2, 3, 4, 7]], 2 * one,
        )
        dh = dy + back_norm(by_a)[0]
        dg1, du1, fu2, sg2 = run(
            "back_0", 6, T, [dh, wd1, gate1, up1], [fixed(tok), down_by(B, D), across(N, B), across(N, B)],
            [wide] * 2, [across(N, B)] * 2, back, [SumA(gu2), SumB(fg2)], [[0, 3, 4, 9, 10], [0, 2, 3, 5, 6, 13]], one,
        )
        gd1, su2 = run(
            "grad_down_0", 7, T, [hid1, dh], [across(N, B), fixed(tok)], [ffd], [down_by(B, D)], grad_down,
            [SumB(fu2)], [[0, 3, 4, 6, 7, 13]], one,
        )
        gg1, gu1, fd1 = run(
            "grad_two_0", 8, T, [a1.T, dg1, du1], [fixed((D, N)), across(N, B), across(N, B)],
            [shape(D, FF)] * 2, [across(D, B)] * 2, grad_two, [SumA(gd1)], [[0, 3, 4, 9, 10]], 2 * one,
        )
        fg1, fu1, sd1 = run("sum_a", 9, 1, [], [], [], [], None, [SumA(gg1), SumA(gu1), SumB(fd1)], flops=one)
        sg1, su1 = run("sum_b", 10, 1, [], [], [], [], None, [SumB(fg1), SumB(fu1)], flops=one)

        sums = [(sg1, sg2), (su1, su2), (sd1, sd2)]
        gradients = [jnp.stack(pair).astype(F32) for pair in sums]
        new = [adamw(w.astype(F32), mm, vv, g) for w, mm, vv, g in zip((wg, wu, wd), m, v, gradients, strict=True)]
        return tuple(one_[which] for which in range(3) for one_ in new)

    states, cut = P(("rep", "r", "s"), None, None), P(None, "s", None)
    return jax.shard_map(
        step,
        mesh=mesh,
        in_specs=(states, states) + (cut,) * 9,
        out_specs=(P("rep", "s", None),) * 9,
        check_vma=False,
    )
```

```python
import functools

import jax
import jax.numpy as jnp
from jax import lax
from jax.experimental import pallas as pl
from jax.experimental.pallas import tpu as pltpu
from jax.sharding import PartitionSpec as P

BF, F32 = jnp.bfloat16, jnp.float32
MESH = pl.DeviceIdType.MESH
ANY = pl.BlockSpec(memory_space=pl.ANY)
TT, UU, VV = 0, 1, 2


def place():
    s = lax.axis_index("s")
    return lax.axis_index("r"), s // 8, (s // 2) % 4, s % 2


def at_s(y, z, c):
    return {"s": (y * 4 + z) * 2 + c}


def step_to(k, d):
    return lax.rem(k + d + 4, 4)


def mate(order, which, d):
    _, y, z, c = place()
    along_y = (order == 0) == (which == 0)
    return at_s(step_to(y, d), z, c) if along_y else at_s(y, step_to(z, d), c)


def partner():
    _, y, z, c = place()
    return at_s(y, z, 1 - c)


def remote(src, dst, send, recv, to):
    return pltpu.make_async_remote_copy(src_ref=src, dst_ref=dst, send_sem=send, recv_sem=recv, device_id=to, device_id_type=MESH)


class Gather:
    far = False

    def __init__(self, order, shard):
        self.order = order
        rows, cols = shard.shape
        self.rows, self.cols = rows, cols
        self.inputs = [shard]
        self.outs = [jax.ShapeDtypeStruct((4, 4, 2, rows, cols), BF)]
        self.out_specs = [ANY]
        self.scratch = [pltpu.VMEM((rows, cols), BF), pltpu.SemaphoreType.DMA((27,)), pltpu.SemaphoreType.DMA((27,)), pltpu.SemaphoreType.DMA((2,))]

    def events(self, ins, outs, scratch):
        (own,), (full,) = ins, outs
        hold, ss, rs, local = scratch
        o, half = self.order, self.cols // 2
        _, y, z, c = place()
        f, g = (y, z) if o == 0 else (z, y)

        def block(fk, gk, core):
            return full.at[fk, gk, core] if o == 0 else full.at[gk, fk, core]

        def column(gk, core):
            return full.at[:, gk, core] if o == 0 else full.at[gk, :, core]

        lo, hi = pl.ds(0, half), pl.ds(half, half)
        fp, fm, f2 = step_to(f, 1), step_to(f, -1), step_to(f, 2)
        gp, gm, g2 = step_to(g, 1), step_to(g, -1), step_to(g, 2)
        me = block(f, g, c)

        up1, dn1 = mate(o, 0, 1), mate(o, 0, -1)
        up2, dn2 = mate(o, 1, 1), mate(o, 1, -1)
        p = partner()

        def half_of(fk, gk, part):
            return full.at[fk, gk, c, :, part] if o == 0 else full.at[gk, fk, c, :, part]

        line = (f, fm, fp, f2)
        table = [
            (own, me, block(fm, g, c), up1),
            (own, me, block(fp, g, c), dn1),
            (own, me, block(f, gm, c), up2),
            (own, me, block(f, gp, c), dn2),
            (half_of(fm, g, lo), half_of(fm, g, lo), half_of(f2, g, lo), up1),
            (half_of(fp, g, hi), half_of(fp, g, hi), half_of(f2, g, hi), dn1),
        ]
        for k in line[1:]:
            table.append((block(k, g, c), block(k, g, c), block(k, gm, c), up2))
            table.append((block(k, g, c), block(k, g, c), block(k, gp, c), dn2))
        for k in line:
            table.append((half_of(k, gm, lo), half_of(k, gm, lo), half_of(k, g2, lo), up2))
        for k in line:
            table.append((half_of(k, gp, hi), half_of(k, gp, hi), half_of(k, g2, hi), dn2))
        table.append((own, me, block(f, g, 1 - c), p))
        for k in line[1:]:
            table.append((block(k, g, c), block(k, g, c), block(k, g, 1 - c), p))
        for k in (gm, gp, g2):
            table.append((column(k, c), column(k, c), column(k, 1 - c), p))

        def start(*numbers):
            for n in numbers:
                src, dst, _, to = table[n]
                remote(src, dst, ss.at[n], rs.at[n], to).start()

        def arrived(*numbers):
            for n in numbers:
                _, _, here, to = table[n]
                remote(here, here, ss.at[n], rs.at[n], to).wait_recv()

        def e0():
            start(0, 1, 2, 3, 20)
            pltpu.make_async_copy(own, hold, local.at[0]).start()

        def e1():
            pltpu.make_async_copy(own, hold, local.at[0]).wait()
            pltpu.make_async_copy(hold, me, local.at[1]).start()
            arrived(0, 1)
            start(4, 5, 6, 7, 8, 9, 21, 22)

        def e2():
            arrived(2, 3)
            start(12, 16)

        def e3():
            arrived(4, 5)
            start(10, 11, 23)

        def e4():
            arrived(6, 7, 8, 9)
            start(13, 17, 14, 18)

        def e5():
            arrived(10, 11)
            start(15, 19, 24, 25)

        def e6():
            arrived(*range(12, 20))
            start(26)

        def e7():
            pltpu.make_async_copy(hold, me, local.at[1]).wait()
            arrived(*range(20, 27))
            for n in range(27):
                src, dst, _, to = table[n]
                remote(src, dst, ss.at[n], rs.at[n], to).wait_send()

        return [e0, e1, e2, e3, e4, e5, e6, e7]


def added(*refs_at):
    total = refs_at[0].astype(F32)
    for r in refs_at[1:]:
        total = total + r.astype(F32)
    return total.astype(BF)


class Ring:
    def __init__(self, slot, n, got, ss, rs, k, up, down):
        self.slot, self.n, self.got, self.ss, self.rs = slot, n, got, ss, rs
        self.k, self.up, self.down = k, up, down

    def copy(self, kind, d):
        k, a = self.k, d
        if kind == TT:
            src = self.slot(a, step_to(k, 2))
        elif kind == UU:
            src = self.slot(1 - a, step_to(k, 1 - 2 * d))
        else:
            src = self.slot(a, step_to(k, 1 - 2 * d))
        return remote(src, self.got.at[kind, d], self.ss.at[kind, d], self.rs.at[kind, d], self.down if d else self.up)

    def first(self):
        for d in (0, 1):
            self.copy(TT, d).start()
        for d in (0, 1):
            self.copy(UU, d).start()

    def second_add(self):
        for d in (0, 1):
            self.copy(TT, d).wait_recv()
        for d in (0, 1):
            ref = self.slot(d, step_to(self.k, 1 - 2 * d))
            for i in range(self.n):
                ref[i] = added(ref[i], self.got[TT, d, i])

    def second_send(self):
        for d in (0, 1):
            self.copy(VV, d).start()

    def last(self, out):
        for kind in (UU, VV):
            for d in (0, 1):
                self.copy(kind, d).wait_recv()
        for a in (0, 1):
            ref = self.slot(a, self.k)
            for i in range(self.n):
                out(a, i, added(ref[i], self.got[VV, a, i], self.got[UU, 1 - a, i]))

    def drain(self):
        for kind in (TT, UU, VV):
            for d in (0, 1):
                self.copy(kind, d).wait_send()


class SumA:
    far = False

    def __init__(self, grad):
        rows, cols = grad.shape
        self.R, self.C = rows // 32, cols // 4
        R, C = self.R, self.C
        self.inputs = [grad.reshape(4, 4, 2, R, cols)]
        self.outs = [jax.ShapeDtypeStruct((2, 2, 4, R, C), BF)]
        self.out_specs = [ANY]
        D = pltpu.SemaphoreType.DMA
        self.scratch = [pltpu.VMEM((4, 4, 4, R, C), BF), pltpu.VMEM((4, 4, 4, R, C), BF), pltpu.VMEM((2, 3, 2, 4, R, C), BF), pltpu.VMEM((2, 2, 4, R, C), BF)]
        self.scratch += [D((4,)), D((4,)), D((4,)), D((2, 3, 2)), D((2, 3, 2)), D]

    def events(self, ins, outs, scratch):
        (g,), (out,) = ins, outs
        H, other, got, F, ls, ds, dr, ss, rs, os = scratch
        C = self.C
        _, y, z, c = place()

        def load(q):
            return pltpu.make_async_copy(g.at[:, :, c, :, pl.ds(q * C, C)], H.at[q], ls.at[q])

        def cross(q):
            return remote(g.at[:, :, 1 - c, :, pl.ds(q * C, C)], other.at[q], ds.at[q], dr.at[q], partner())

        def slot(o):
            return lambda ab, k: H.at[2 * o + ab, k] if o == 0 else H.at[2 * o + ab, :, k]

        rings = [Ring(slot(o), 4, got.at[o], ss.at[o], rs.at[o], (y, z)[o], mate(o, 0, 1), mate(o, 0, -1)) for o in (0, 1)]

        def e0():
            for q in range(4):
                cross(q).start()
                load(q).start()

        def e1():
            for q in range(4):
                load(q).wait()
                cross(q).wait_recv()

                def body(a, _):
                    for b in range(4):
                        H[q, a, b] = added(H[q, a, b], other[q, a, b])
                    return 0

                lax.fori_loop(0, 4, body, 0)

        def e2():
            for r in rings:
                r.first()

        def e3():
            for r in rings:
                r.second_add()

        def e4():
            for r in rings:
                r.second_send()

        def e5():
            for o, r in enumerate(rings):

                def put(a, i, value, o=o):
                    F[o, a, i] = value

                r.last(put)

        def e6():
            if out is not None:
                pltpu.make_async_copy(F, out, os).start()
            for r in rings:
                r.drain()
            for q in range(4):
                cross(q).wait_send()
            if out is not None:
                pltpu.make_async_copy(F, out, os).wait()

        return [e0, e1, e2, e3, e4, e5, e6]


class SumB:
    far = True

    def __init__(self, part, dims=None):
        R, C = dims or part.shape[3:]
        self.R, self.C = R, C
        self.inputs = [part]
        self.outs = [jax.ShapeDtypeStruct((R, 4 * C), BF)]
        self.out_specs = [ANY]
        D = pltpu.SemaphoreType.DMA
        self.scratch = [pltpu.VMEM((2, 2, 4, R, C), BF), pltpu.VMEM((2, 3, 2, 1, R, C), BF), pltpu.VMEM((4, R, C), BF), pltpu.VMEM((4, R, C), BF), pltpu.VMEM((4, R, C), BF)]
        self.scratch += [D, D((2, 3, 2)), D((2, 3, 2)), D((2, 3)), D((2, 3)), D((4,))]

    def events(self, ins, outs, scratch, held=None):
        (part,), (out,) = ins, outs
        F, got, E, X, G, ls, ss, rs, xs, xr, os = scratch
        F = F if held is None else held
        C = self.C
        x, y, z, c = place()

        def slot(o):
            return lambda ab, k: F.at[o, ab, pl.ds(k, 1)]

        rings = [Ring(slot(o), 1, got.at[o], ss.at[o], rs.at[o], (z, y)[o], mate(o, 1, 1), mate(o, 1, -1)) for o in (0, 1)]

        def over(d):
            return remote(E.at[step_to(x, d)], X.at[x], xs.at[0, d - 1], xr.at[0, d - 1], {"r": step_to(x, d)})

        def over_came(d):
            here = X.at[step_to(x, -d)]
            return remote(here, here, xs.at[0, d - 1], xr.at[0, d - 1], {"r": step_to(x, d)})

        def share(d):
            return remote(G.at[x], G.at[x], xs.at[1, d - 1], xr.at[1, d - 1], {"r": step_to(x, d)})

        def share_came(d):
            here = G.at[step_to(x, -d)]
            return remote(here, here, xs.at[1, d - 1], xr.at[1, d - 1], {"r": step_to(x, d)})

        def store(q):
            return pltpu.make_async_copy(G.at[q], out.at[:, pl.ds(q * C, C)], os.at[q])

        def e0():
            if held is None:
                pltpu.make_async_copy(part, F, ls).start()
                pltpu.make_async_copy(part, F, ls).wait()
            for r in rings:
                r.first()

        def e1():
            for r in rings:
                r.second_add()

        def e2():
            for r in rings:
                r.second_send()

        def e3():
            for o, r in enumerate(rings):

                def put(a, i, value, o=o):
                    E[2 * o + a] = value

                r.last(put)
            X[x] = E[x]

        def e4():
            for d in (2, 1, 3):
                over(d).start()

        def e5():
            for d in (1, 3, 2):
                over_came(d).wait_recv()
            G[x] = added(*(X[i] for i in range(4)))

        def e6():
            for d in (2, 1, 3):
                share(d).start()

        def e7():
            for d in (1, 3, 2):
                share_came(d).wait_recv()
            for q in range(4):
                store(q).start()
            for r in rings:
                r.drain()
            for d in (1, 3, 2):
                over(d).wait_send()
                share(d).wait_send()
            for q in range(4):
                store(q).wait()

        return [e0, e1, e2, e3, e4, e5, e6, e7]


class Sum:
    far = True

    def __init__(self, grad):
        self.a = SumA(grad)
        self.b = SumB(None, (self.a.R, self.a.C))
        self.inputs, self.outs, self.out_specs = self.a.inputs, self.b.outs, self.b.out_specs
        self.scratch = self.a.scratch + self.b.scratch

    def events(self, ins, outs, scratch):
        n = len(self.a.scratch)
        first = self.a.events(ins, [None], scratch[:n])
        second = self.b.events([None], outs, scratch[n:], held=scratch[3])
        return first[:-1] + second + first[-1:]


def run(name, number, steps, arrays, specs, outs, out_specs, compute, jobs=(), when=None, flops=0, hold=(), order=None):
    n_in, n_out = len(arrays), len(outs)
    job_in = [a for j in jobs for a in j.inputs]
    job_out = [a for j in jobs for a in j.outs]

    def body(*refs):
        ins, rest = refs[:n_in], refs[n_in:]
        jin, rest = rest[: len(job_in)], rest[len(job_in) :]
        mouts, rest = rest[:n_out], rest[n_out:]
        jout, scratch = rest[: len(job_out)], rest[len(job_out) :]
        held, scratch = scratch[: len(hold)], scratch[len(hold) :]
        t = pl.program_id(0)
        lists = []
        for j in jobs:
            a, jin = jin[: len(j.inputs)], jin[len(j.inputs) :]
            b, jout = jout[: len(j.outs)], jout[len(j.outs) :]
            c, scratch = scratch[: len(j.scratch)], scratch[len(j.scratch) :]
            lists.append(j.events(a, b, c))
        if jobs:

            @pl.when(t == 0)
            def _():
                barrier = pltpu.get_barrier_semaphore()
                them = [mate(0, w, d) for w in (0, 1) for d in (1, -1)] + [partner()]
                if any(j.far for j in jobs):
                    x = lax.axis_index("r")
                    them += [{"r": step_to(x, d)} for d in (1, 2, 3)]
                for device in them:
                    pl.semaphore_signal(barrier, inc=1, device_id=device, device_id_type=MESH)
                pl.semaphore_wait(barrier, len(them))

        table = {}
        for j, events in enumerate(lists):
            for i, e in enumerate(events):
                at = when[j][i] if when and i < len(when[j]) else steps
                table.setdefault(min(at, steps), []).append((i, j, e))
        for at in sorted(table):
            if at < steps:

                @pl.when(t == at)
                def _(at=at):
                    for _, _, e in sorted(table[at], key=lambda v: v[:2]):
                        e()

        if compute is not None:
            compute(t, ins, (*mouts, *held))
        if steps in table:

            @pl.when(t == steps - 1)
            def _():
                late = {(i, j): e for i, j, e in table[steps]}
                for key in [(i, j) for j, i in order] if order else sorted(late):
                    late[key]()

    got = pl.pallas_call(
        body,
        name=name,
        grid=(steps,),
        out_shape=list(outs) + job_out,
        in_specs=list(specs) + [ANY] * len(job_in),
        out_specs=list(out_specs) + [s for j in jobs for s in j.out_specs],
        scratch_shapes=list(hold) + [s for j in jobs for s in j.scratch],
        compiler_params=pltpu.CompilerParams(
            dimension_semantics=("arbitrary",),
            vmem_limit_bytes=66_000_000,
            **(dict(collective_id=number, has_side_effects=True) if jobs else {}),
        ),
        cost_estimate=pl.CostEstimate(flops=flops, bytes_accessed=50_000_000, transcendentals=0),
    )(*arrays, *job_in)
    return list(got)


def fixed(shape):
    return pl.BlockSpec(shape, lambda t: (0,) * len(shape), pipeline_mode=pl.Buffered(1))


def across(rows, cols):
    return pl.BlockSpec((rows, cols), lambda t: (0, t))


def down_by(rows, cols):
    return pl.BlockSpec((rows, cols), lambda t: (t, 0))


def nn(a, b):
    return jnp.dot(a, b, preferred_element_type=F32)


def nt(a, b):
    return lax.dot_general(a, b, (((1,), (1,)), ((), ())), preferred_element_type=F32)


def tn(a, b):
    return lax.dot_general(a, b, (((0,), (0,)), ((), ())), preferred_element_type=F32)


def shape(*dims, dtype=BF):
    return jax.ShapeDtypeStruct(dims, dtype)


def by_rows(total, ROWS, fn):
    if total == ROWS:
        return fn(slice(None))

    def body(i, _):
        fn(pl.ds(pl.multiple_of(i * ROWS, ROWS), ROWS))
        return 0

    lax.fori_loop(0, total // ROWS, body, 0)


def glu(t, ins, outs):
    a, wg, wu = ins
    gate_ref, up_ref, hid_ref = outs

    def part(rows):
        gate, up = nn(a[rows, :], wg[...]), nn(a[rows, :], wu[...])
        gate_ref[rows, :] = gate
        up_ref[rows, :] = up
        hid_ref[rows, :] = (gate * jax.nn.sigmoid(gate) * up).astype(BF)

    by_rows(a.shape[0], a.shape[0], part)


def glu_back(by_hid, gate, up):
    by_hid = by_hid.astype(BF).astype(F32)
    sig = jax.nn.sigmoid(gate)
    act = gate * sig
    return (act * up).astype(BF), (by_hid * up * (sig + act * (1.0 - sig))).astype(BF), (by_hid * act).astype(BF)


def both_ways(t, ins, outs):
    a, dy, wg, wu, wd = ins
    dg_ref, du_ref, gd_ref, hid_ref = outs

    def part(rows):
        gate, up = nn(a[rows, :], wg[...]), nn(a[rows, :], wu[...])
        hid_ref[rows, :], dg_ref[rows, :], du_ref[rows, :] = glu_back(nt(dy[rows, :], wd[...]), gate, up)

    by_rows(a.shape[0], 1024, part)
    gd_ref[...] = tn(hid_ref[...], dy[...]).astype(BF)


def back(t, ins, outs):
    dy, wd, gate, up, hid = ins
    dg_ref, du_ref, gd_ref = outs

    def part(rows):
        _, dg_ref[rows, :], du_ref[rows, :] = glu_back(nt(dy[rows, :], wd[...]), gate[rows, :], up[rows, :])

    by_rows(dy.shape[0], 512, part)
    gd_ref[...] = tn(hid[...], dy[...]).astype(BF)


def normed(h):
    wide = h.astype(F32)
    scale = lax.rsqrt(jnp.mean(wide**2, -1, keepdims=True) + 1e-6)
    return (wide * scale).astype(BF)


def norm(t, ins, outs):
    outs[0][...] = normed(ins[0][...])


def lower(t, ins, outs):
    hid, wd, h = ins
    below = h[...] + nn(hid[...], wd[...]).astype(BF)
    outs[0][...] = below
    outs[1][...] = normed(below)


def grad_two(t, ins, outs):
    a, dg, du = ins
    outs[0][...] = tn(a[...], dg[...]).astype(BF)
    outs[1][...] = tn(a[...], du[...]).astype(BF)


def grad_a(t, ins, outs):
    dg, du, wg, wu, h, dy = ins
    by_a = (nt(dg[...], wg[...]).astype(BF) + nt(du[...], wu[...]).astype(BF)).astype(F32)
    wide = h[...].astype(F32)
    scale = lax.rsqrt(jnp.mean(wide**2, -1, keepdims=True) + 1e-6)
    along = jnp.mean(by_a * wide, -1, keepdims=True)
    by_h = by_a * scale - wide * (along * scale * scale * scale)
    outs[0][...] = dy[...] + by_h.astype(BF)


def adamw(w, m, v, g):
    m = 0.9 * m + 0.1 * g
    v = 0.95 * v + 0.05 * g * g
    step = m * lax.rsqrt(v + 1e-8) + 0.1 * w
    return (w - 0.02 * step).astype(BF), m, v


def solution(mesh):
    def step(x, dy, *arrays):
        (wg, wu, wd), m, v = (arrays[i : i + 3] for i in (0, 3, 6))
        N, D = x.shape[1:]
        FF = wg.shape[2]
        B, TB = 256, 256
        T, TN = FF // B, N // TB
        one = 2 * N * D * FF
        flat = lambda w: w.reshape(-1, w.shape[-1])
        wide, tokens = shape(N, FF), shape(N, D)
        whole = fixed((N, D))
        raw_whole = pl.BlockSpec((None, N, D), lambda t: (0, 0, 0), pipeline_mode=pl.Buffered(1))
        raw_rows = pl.BlockSpec((None, TB, D), lambda t: (0, t, 0))
        rows = down_by(TB, D)

        a1, wg1, wu1 = run("fetch_0", 1, TN, [x], [raw_rows], [tokens], [rows], norm, [Gather(0, wg[0]), Gather(1, wu[0])], [[0], [0]], one)
        gate1, up1, hid1, wd1, wg2 = run(
            "glu_0", 2, T, [a1, flat(wg1), flat(wu1)], [whole, across(D, B), across(D, B)],
            [shape(N, FF, dtype=F32), shape(N, FF, dtype=F32), wide], [across(N, B)] * 3, glu,
            [Gather(0, wd[0]), Gather(1, wg[1])], [[0, 2, 3, 4, 6, 8, 11]] * 2, 2 * one,
        )
        wd1, wg2 = flat(wd1), flat(wg2)
        h1, a2, wu2, wd2 = run(
            "lower_0", 3, TN, [hid1, wd1, x], [down_by(TB, FF), fixed((FF, D)), raw_rows],
            [tokens] * 2, [rows] * 2, lower, [Gather(0, wu[1]), Gather(1, wd[1])], [[0, 2, 3, 4, 5, 7]] * 2, one,
        )
        wu2, wd2 = flat(wu2), flat(wd2)
        dg2, du2, gd2 = run(
            "both_1", 0, T, [a2, dy, wg2, wu2, wd2], [whole, raw_whole, across(D, B), across(D, B), down_by(B, D)],
            [wide, wide, shape(FF, D)], [across(N, B)] * 2 + [down_by(B, D)], both_ways, flops=4 * one, hold=[pltpu.VMEM((N, B), BF)],
        )
        gg2, gu2, fd2 = run(
            "grad_two_1", 4, T, [a2, dg2, du2], [whole, across(N, B), across(N, B)],
            [shape(D, FF)] * 2, [across(D, B)] * 2, grad_two, [SumA(gd2)], [[0, 3, 3, 8, 8, 11]], 2 * one,
        )
        dh, fg2, sd2 = run(
            "grad_a_1", 5, TN, [dg2, du2, wg2, wu2, h1, dy], [down_by(TB, FF)] * 2 + [fixed((D, FF))] * 2 + [rows, raw_rows],
            [tokens], [rows], grad_a, [SumA(gg2), SumB(fd2)], [[0, 2, 2, 5, 5, 7], [0, 1, 1, 3, 3, 4, 4, 6]], 2 * one,
        )
        dg1, du1, gd1, fu2, sg2 = run(
            "back_0", 6, T, [dh, wd1, gate1, up1, hid1], [whole, down_by(B, D)] + [across(N, B)] * 3,
            [wide, wide, shape(FF, D)], [across(N, B)] * 2 + [down_by(B, D)], back,
            [SumA(gu2), SumB(fg2)], [[0, 2, 2, 6, 6, 9, 11], [0, 1, 1, 3, 3, 5, 5, 8]], 2 * one,
        )
        gg1, gu1, fd1, su2 = run(
            "grad_two_0", 7, T, [a1, dg1, du1], [whole, across(N, B), across(N, B)],
            [shape(D, FF)] * 2, [across(D, B)] * 2, grad_two, [SumA(gd1), SumB(fu2)], [[0, 3, 3, 8, 8, 11], [0, 2, 2, 5, 5, 7, 7, 10]], 2 * one,
        )
        order = [(0, 0), (1, 0), (2, 0), (0, 1), (0, 2), (2, 1), (2, 2), (1, 1), (1, 2), (2, 3), (2, 4), (0, 3), (0, 4), (2, 5), (2, 6)]
        order += [(1, 3), (1, 4), (0, 5), (0, 6), (1, 5), (1, 6), (2, 7), (0, 7), (0, 8), (1, 7), (1, 8), (0, 9), (0, 10), (1, 9), (1, 10)]
        order += [(0, 11), (0, 12), (1, 11), (1, 12), (0, 13), (1, 13), (0, 14), (1, 14)]
        sg1, su1, sd1 = run("sum_last", 8, 1, [], [], [], [], None, [Sum(gg1), Sum(gu1), SumB(fd1)], flops=one, order=order)

        sums = [(sg1, sg2), (su1, su2), (sd1, sd2)]
        gradients = [jnp.stack(pair).astype(F32) for pair in sums]
        new = [adamw(w.astype(F32), mm, vv, g) for w, mm, vv, g in zip((wg, wu, wd), m, v, gradients, strict=True)]
        return tuple(one_[which] for which in range(3) for one_ in new)

    states, cut = P(("rep", "r", "s"), None, None), P(None, "s", None)
    return jax.shard_map(
        step,
        mesh=mesh,
        in_specs=(states, states) + (cut,) * 9,
        out_specs=(P("rep", "s", None),) * 9,
        check_vma=False,
    )
```

```python
import functools

import jax
import jax.numpy as jnp
from jax import lax
from jax.experimental import pallas as pl
from jax.experimental.pallas import tpu as pltpu
from jax.sharding import PartitionSpec as P

BF, F32 = jnp.bfloat16, jnp.float32
MESH = pl.DeviceIdType.MESH
ANY = pl.BlockSpec(memory_space=pl.ANY)
TT, UU, VV = 0, 1, 2


def place():
    s = lax.axis_index("s")
    return lax.axis_index("r"), s // 8, (s // 2) % 4, s % 2


def at_s(y, z, c):
    return {"s": (y * 4 + z) * 2 + c}


def step_to(k, d):
    return lax.rem(k + d + 4, 4)


def mate(order, which, d):
    _, y, z, c = place()
    along_y = (order == 0) == (which == 0)
    return at_s(step_to(y, d), z, c) if along_y else at_s(y, step_to(z, d), c)


def partner():
    _, y, z, c = place()
    return at_s(y, z, 1 - c)


def remote(src, dst, send, recv, to):
    return pltpu.make_async_remote_copy(src_ref=src, dst_ref=dst, send_sem=send, recv_sem=recv, device_id=to, device_id_type=MESH)


class Gather:
    far, pair = False, 0

    def __init__(self, order, shards, layer):
        self.order, self.layer = order, layer
        _, rows, cols = shards.shape
        self.rows, self.cols = rows, cols
        self.inputs = [shards]
        self.outs = [jax.ShapeDtypeStruct((4, 4, 2, rows, cols), BF)]
        self.out_specs = [ANY]
        self.scratch = [pltpu.VMEM((rows, cols), BF), pltpu.SemaphoreType.DMA((27,)), pltpu.SemaphoreType.DMA((27,)), pltpu.SemaphoreType.DMA((2,))]

    def events(self, ins, outs, scratch):
        (own,), (full,) = ins, outs
        own = own.at[self.layer]
        hold, ss, rs, local = scratch
        o, half = self.order, self.cols // 2
        _, y, z, c = place()
        f, g = (y, z) if o == 0 else (z, y)

        def block(fk, gk, core):
            return full.at[fk, gk, core] if o == 0 else full.at[gk, fk, core]

        def column(gk, core):
            return full.at[:, gk, core] if o == 0 else full.at[gk, :, core]

        lo, hi = pl.ds(0, half), pl.ds(half, half)
        fp, fm, f2 = step_to(f, 1), step_to(f, -1), step_to(f, 2)
        gp, gm, g2 = step_to(g, 1), step_to(g, -1), step_to(g, 2)
        me = block(f, g, c)

        up1, dn1 = mate(o, 0, 1), mate(o, 0, -1)
        up2, dn2 = mate(o, 1, 1), mate(o, 1, -1)
        p = partner()

        def half_of(fk, gk, part):
            return full.at[fk, gk, c, :, part] if o == 0 else full.at[gk, fk, c, :, part]

        line = (f, fm, fp, f2)
        table = [
            (own, me, block(fm, g, c), up1),
            (own, me, block(fp, g, c), dn1),
            (own, me, block(f, gm, c), up2),
            (own, me, block(f, gp, c), dn2),
            (half_of(fm, g, lo), half_of(fm, g, lo), half_of(f2, g, lo), up1),
            (half_of(fp, g, hi), half_of(fp, g, hi), half_of(f2, g, hi), dn1),
        ]
        for k in line[1:]:
            table.append((block(k, g, c), block(k, g, c), block(k, gm, c), up2))
            table.append((block(k, g, c), block(k, g, c), block(k, gp, c), dn2))
        for k in line:
            table.append((half_of(k, gm, lo), half_of(k, gm, lo), half_of(k, g2, lo), up2))
        for k in line:
            table.append((half_of(k, gp, hi), half_of(k, gp, hi), half_of(k, g2, hi), dn2))
        table.append((own, me, block(f, g, 1 - c), p))
        for k in line[1:]:
            table.append((block(k, g, c), block(k, g, c), block(k, g, 1 - c), p))
        for k in (gm, gp, g2):
            table.append((column(k, c), column(k, c), column(k, 1 - c), p))

        def start(*numbers):
            for n in numbers:
                src, dst, _, to = table[n]
                remote(src, dst, ss.at[n], rs.at[n], to).start()

        def arrived(*numbers):
            for n in numbers:
                _, _, here, to = table[n]
                remote(here, here, ss.at[n], rs.at[n], to).wait_recv()

        def e0():
            start(0, 1, 2, 3, 20)
            pltpu.make_async_copy(own, hold, local.at[0]).start()

        def e1():
            pltpu.make_async_copy(own, hold, local.at[0]).wait()
            pltpu.make_async_copy(hold, me, local.at[1]).start()
            arrived(0, 1)
            start(4, 5, 6, 7, 8, 9, 21, 22)

        def e2():
            arrived(2, 3)
            start(12, 16)

        def e3():
            arrived(4, 5)
            start(10, 11, 23)

        def e4():
            arrived(6, 7, 8, 9)
            start(13, 17, 14, 18)

        def e5():
            arrived(10, 11)
            start(15, 19, 24, 25)

        def e6():
            arrived(*range(12, 20))
            start(26)

        def e7():
            pltpu.make_async_copy(hold, me, local.at[1]).wait()
            arrived(*range(20, 27))
            for n in range(27):
                src, dst, _, to = table[n]
                remote(src, dst, ss.at[n], rs.at[n], to).wait_send()

        return [e0, e1, e2, e3, e4, e5, e6, e7]


def added(*refs_at):
    total = refs_at[0].astype(F32)
    for r in refs_at[1:]:
        total = total + r.astype(F32)
    return total.astype(BF)


class Ring:
    def __init__(self, slot, n, got, ss, rs, k, up, down):
        self.slot, self.n, self.got, self.ss, self.rs = slot, n, got, ss, rs
        self.k, self.up, self.down = k, up, down

    def copy(self, kind, d):
        k, a = self.k, d
        if kind == TT:
            src = self.slot(a, step_to(k, 2))
        elif kind == UU:
            src = self.slot(1 - a, step_to(k, 1 - 2 * d))
        else:
            src = self.slot(a, step_to(k, 1 - 2 * d))
        return remote(src, self.got.at[kind, d], self.ss.at[kind, d], self.rs.at[kind, d], self.down if d else self.up)

    def first(self):
        for d in (0, 1):
            self.copy(TT, d).start()
        for d in (0, 1):
            self.copy(UU, d).start()

    def second_add(self):
        for d in (0, 1):
            self.copy(TT, d).wait_recv()
        for d in (0, 1):
            ref = self.slot(d, step_to(self.k, 1 - 2 * d))
            for i in range(self.n):
                ref[i] = added(ref[i], self.got[TT, d, i])

    def second_send(self):
        for d in (0, 1):
            self.copy(VV, d).start()

    def last(self, out):
        for kind in (UU, VV):
            for d in (0, 1):
                self.copy(kind, d).wait_recv()
        for a in (0, 1):
            ref = self.slot(a, self.k)
            for i in range(self.n):
                out(a, i, added(ref[i], self.got[VV, a, i], self.got[UU, 1 - a, i]))

    def drain(self):
        for kind in (TT, UU, VV):
            for d in (0, 1):
                self.copy(kind, d).wait_send()


class SumA:
    far, pair = False, 1

    def __init__(self, grad):
        rows, cols = grad.shape
        self.R, self.C = rows // 32, cols // 4
        R, C = self.R, self.C
        self.inputs = [grad.reshape(4, 4, 2, R, cols)]
        self.outs = [jax.ShapeDtypeStruct((2, 2, 4, R, C), BF)]
        self.out_specs = [ANY]
        D = pltpu.SemaphoreType.DMA
        self.scratch = [pltpu.VMEM((4, 4, 4, R, C), BF), pltpu.VMEM((4, 4, 4, R, C), BF), pltpu.VMEM((2, 3, 2, 4, R, C), BF), pltpu.VMEM((2, 2, 4, R, C), BF)]
        self.scratch += [D((4,)), D((4,)), D((4,)), D((2, 3, 2)), D((2, 3, 2)), D]

    def events(self, ins, outs, scratch):
        (g,), (out,) = ins, outs
        H, other, got, F, ls, ds, dr, ss, rs, os = scratch
        C = self.C
        _, y, z, c = place()

        def load(q):
            return pltpu.make_async_copy(g.at[:, :, c, :, pl.ds(q * C, C)], H.at[q], ls.at[q])

        def cross(q):
            return remote(g.at[:, :, 1 - c, :, pl.ds(q * C, C)], other.at[q], ds.at[q], dr.at[q], partner())

        def slot(o):
            return lambda ab, k: H.at[2 * o + ab, k] if o == 0 else H.at[2 * o + ab, :, k]

        rings = [Ring(slot(o), 4, got.at[o], ss.at[o], rs.at[o], (y, z)[o], mate(o, 0, 1), mate(o, 0, -1)) for o in (0, 1)]

        def e0():
            for q in range(4):
                cross(q).start()
                load(q).start()

        def e1():
            for q in range(4):
                load(q).wait()
                cross(q).wait_recv()

                def body(a, _):
                    for b in range(4):
                        H[q, a, b] = added(H[q, a, b], other[q, a, b])
                    return 0

                lax.fori_loop(0, 4, body, 0)

        def e2():
            for r in rings:
                r.first()

        def e3():
            for r in rings:
                r.second_add()

        def e4():
            for r in rings:
                r.second_send()

        def e5():
            for o, r in enumerate(rings):

                def put(a, i, value, o=o):
                    F[o, a, i] = value

                r.last(put)

        def e6():
            if out is not None:
                pltpu.make_async_copy(F, out, os).start()
            for r in rings:
                r.drain()
            for q in range(4):
                cross(q).wait_send()
            if out is not None:
                pltpu.make_async_copy(F, out, os).wait()

        return [e0, e1, e2, e3, e4, e5, e6]


class SumB:
    far, pair = True, 1

    def __init__(self, part, dims=None):
        R, C = dims or part.shape[3:]
        self.R, self.C = R, C
        self.inputs = [part]
        self.outs = [jax.ShapeDtypeStruct((R, 4 * C), BF)]
        self.out_specs = [ANY]
        D = pltpu.SemaphoreType.DMA
        self.scratch = [pltpu.VMEM((2, 2, 4, R, C), BF), pltpu.VMEM((2, 3, 2, 1, R, C), BF), pltpu.VMEM((4, R, C), BF), pltpu.VMEM((4, R, C), BF), pltpu.VMEM((4, R, C), BF)]
        self.scratch += [D, D((2, 3, 2)), D((2, 3, 2)), D((2, 3)), D((2, 3)), D((4,))]

    def events(self, ins, outs, scratch, held=None):
        (part,), (out,) = ins, outs
        F, got, E, X, G, ls, ss, rs, xs, xr, os = scratch
        F = F if held is None else held
        C = self.C
        x, y, z, c = place()

        def slot(o):
            return lambda ab, k: F.at[o, ab, pl.ds(k, 1)]

        rings = [Ring(slot(o), 1, got.at[o], ss.at[o], rs.at[o], (z, y)[o], mate(o, 1, 1), mate(o, 1, -1)) for o in (0, 1)]

        def over(d):
            return remote(E.at[step_to(x, d)], X.at[x], xs.at[0, d - 1], xr.at[0, d - 1], {"r": step_to(x, d)})

        def over_came(d):
            here = X.at[step_to(x, -d)]
            return remote(here, here, xs.at[0, d - 1], xr.at[0, d - 1], {"r": step_to(x, d)})

        def share(d):
            return remote(G.at[x], G.at[x], xs.at[1, d - 1], xr.at[1, d - 1], {"r": step_to(x, d)})

        def share_came(d):
            here = G.at[step_to(x, -d)]
            return remote(here, here, xs.at[1, d - 1], xr.at[1, d - 1], {"r": step_to(x, d)})

        def store(q):
            return pltpu.make_async_copy(G.at[q], out.at[:, pl.ds(q * C, C)], os.at[q])

        def e0():
            if held is None:
                pltpu.make_async_copy(part, F, ls).start()
                pltpu.make_async_copy(part, F, ls).wait()
            for r in rings:
                r.first()

        def e1():
            for r in rings:
                r.second_add()

        def e2():
            for r in rings:
                r.second_send()

        def e3():
            for o, r in enumerate(rings):

                def put(a, i, value, o=o):
                    E[2 * o + a] = value

                r.last(put)
            X[x] = E[x]

        def e4():
            for d in (2, 1, 3):
                over(d).start()

        def e5():
            for d in (1, 3, 2):
                over_came(d).wait_recv()
            G[x] = added(*(X[i] for i in range(4)))

        def e6():
            for d in (2, 1, 3):
                share(d).start()

        def e7():
            for d in (1, 3, 2):
                share_came(d).wait_recv()
            for q in range(4):
                store(q).start()
            for r in rings:
                r.drain()
            for d in (1, 3, 2):
                over(d).wait_send()
                share(d).wait_send()
            for q in range(4):
                store(q).wait()

        return [e0, e1, e2, e3, e4, e5, e6, e7]


class Sum:
    far, pair = True, 1

    def __init__(self, grad):
        self.a = SumA(grad)
        self.b = SumB(None, (self.a.R, self.a.C))
        self.inputs, self.outs, self.out_specs = self.a.inputs, self.b.outs, self.b.out_specs
        self.scratch = self.a.scratch + self.b.scratch

    def events(self, ins, outs, scratch):
        n = len(self.a.scratch)
        first = self.a.events(ins, [None], scratch[:n])
        second = self.b.events([None], outs, scratch[n:], held=scratch[3])
        return first[:-1] + second + first[-1:]


def run(name, number, steps, arrays, specs, outs, out_specs, compute, jobs=(), when=None, flops=0, hold=()):
    n_in, n_out = len(arrays), len(outs)
    job_in = [a for j in jobs for a in j.inputs]
    job_out = [a for j in jobs for a in j.outs]

    def body(*refs):
        ins, rest = refs[:n_in], refs[n_in:]
        jin, rest = rest[: len(job_in)], rest[len(job_in) :]
        mouts, rest = rest[:n_out], rest[n_out:]
        jout, scratch = rest[: len(job_out)], rest[len(job_out) :]
        held, scratch = scratch[: len(hold)], scratch[len(hold) :]
        t = pl.program_id(0)
        lists = []
        for j in jobs:
            a, jin = jin[: len(j.inputs)], jin[len(j.inputs) :]
            b, jout = jout[: len(j.outs)], jout[len(j.outs) :]
            c, scratch = scratch[: len(j.scratch)], scratch[len(j.scratch) :]
            lists.append(j.events(a, b, c))
        if jobs:

            @pl.when(t == 0)
            def _():
                barrier = pltpu.get_barrier_semaphore()
                them = [mate(0, w, d) for w in (0, 1) for d in (1, -1)] + [partner()]
                if any(j.far for j in jobs):
                    x = lax.axis_index("r")
                    them += [{"r": step_to(x, d)} for d in (1, 2, 3)]
                for device in them:
                    pl.semaphore_signal(barrier, inc=1, device_id=device, device_id_type=MESH)
                pl.semaphore_wait(barrier, len(them))

        def turn(entry):
            i, j, _ = entry
            pair = jobs[j].pair
            return (i + pair) // (1 + pair), j, i

        table = {}
        for j, events in enumerate(lists):
            for i, e in enumerate(events):
                at = int(when[j][i], 36) if when and i < len(when[j]) else steps
                table.setdefault(min(at, steps), []).append((i, j, e))
        for at in sorted(table):
            if at < steps:

                @pl.when(t == at)
                def _(at=at):
                    for _, _, e in sorted(table[at], key=turn):
                        e()

        if compute is not None:
            compute(t, ins, (*mouts, *held))
        if steps in table:

            @pl.when(t == steps - 1)
            def _():
                for _, _, e in sorted(table[steps], key=turn):
                    e()

    got = pl.pallas_call(
        body,
        name=name,
        grid=(steps,),
        out_shape=list(outs) + job_out,
        in_specs=list(specs) + [ANY] * len(job_in),
        out_specs=list(out_specs) + [s for j in jobs for s in j.out_specs],
        scratch_shapes=list(hold) + [s for j in jobs for s in j.scratch],
        compiler_params=pltpu.CompilerParams(
            dimension_semantics=("arbitrary",),
            vmem_limit_bytes=66_000_000,
            **(dict(collective_id=number, has_side_effects=True) if jobs else {}),
        ),
        cost_estimate=pl.CostEstimate(flops=flops, bytes_accessed=50_000_000, transcendentals=0),
    )(*arrays, *job_in)
    return list(got)


def fixed(shape):
    return pl.BlockSpec(shape, lambda t: (0,) * len(shape), pipeline_mode=pl.Buffered(1))


def across(rows, cols):
    return pl.BlockSpec((rows, cols), lambda t: (0, t))


def down_by(rows, cols):
    return pl.BlockSpec((rows, cols), lambda t: (t, 0))


def nn(a, b):
    return jnp.dot(a, b, preferred_element_type=F32)


def nt(a, b):
    return lax.dot_general(a, b, (((1,), (1,)), ((), ())), preferred_element_type=F32)


def tn(a, b):
    return lax.dot_general(a, b, (((0,), (0,)), ((), ())), preferred_element_type=F32)


def shape(*dims, dtype=BF):
    return jax.ShapeDtypeStruct(dims, dtype)


def by_rows(total, ROWS, fn):
    if total == ROWS:
        return fn(slice(None))

    def body(i, _):
        fn(pl.ds(pl.multiple_of(i * ROWS, ROWS), ROWS))
        return 0

    lax.fori_loop(0, total // ROWS, body, 0)


def glu(t, ins, outs):
    a, wg, wu = ins
    gate_ref, up_ref, hid_ref = outs
    gate, up = nn(a[...], wg[...]), nn(a[...], wu[...])
    gate_ref[...] = gate
    up_ref[...] = up
    hid_ref[...] = (gate * jax.nn.sigmoid(gate) * up).astype(BF)


def glu_back(by_hid, gate, up):
    by_hid = by_hid.astype(BF).astype(F32)
    sig = jax.nn.sigmoid(gate)
    act = gate * sig
    return (act * up).astype(BF), (by_hid * up * (sig + act * (1.0 - sig))).astype(BF), (by_hid * act).astype(BF)


def both_ways(t, ins, outs):
    a, dy, wg, wu, wd = ins
    dg_ref, du_ref, gd_ref, hid_ref = outs

    def part(rows):
        gate, up = nn(a[rows, :], wg[...]), nn(a[rows, :], wu[...])
        hid_ref[rows, :], dg_ref[rows, :], du_ref[rows, :] = glu_back(nt(dy[rows, :], wd[...]), gate, up)

    by_rows(a.shape[0], 1024, part)
    gd_ref[...] = tn(hid_ref[...], dy[...]).astype(BF)


def back(t, ins, outs):
    dy, wd, gate, up, hid = ins
    dg_ref, du_ref, gd_ref = outs

    def part(rows):
        _, dg_ref[rows, :], du_ref[rows, :] = glu_back(nt(dy[rows, :], wd[...]), gate[rows, :], up[rows, :])

    by_rows(dy.shape[0], 512, part)
    gd_ref[...] = tn(hid[...], dy[...]).astype(BF)


def normed(h):
    wide = h.astype(F32)
    scale = lax.rsqrt(jnp.mean(wide**2, -1, keepdims=True) + 1e-6)
    return (wide * scale).astype(BF)


def norm(t, ins, outs):
    outs[0][...] = normed(ins[0][...])


def lower(t, ins, outs):
    hid, wd, h = ins
    below = h[...] + nn(hid[...], wd[...]).astype(BF)
    outs[0][...] = below
    outs[1][...] = normed(below)


def grad_two(t, ins, outs):
    a, dg, du = ins
    outs[0][...] = tn(a[...], dg[...]).astype(BF)
    outs[1][...] = tn(a[...], du[...]).astype(BF)


def grad_a(t, ins, outs):
    dg, du, wg, wu, h, dy = ins
    by_a = (nt(dg[...], wg[...]).astype(BF) + nt(du[...], wu[...]).astype(BF)).astype(F32)
    wide = h[...].astype(F32)
    scale = lax.rsqrt(jnp.mean(wide**2, -1, keepdims=True) + 1e-6)
    along = jnp.mean(by_a * wide, -1, keepdims=True)
    by_h = by_a * scale - wide * (along * scale * scale * scale)
    outs[0][...] = dy[...] + by_h.astype(BF)


def adamw(w, m, v, g):
    m = 0.9 * m + 0.1 * g
    v = 0.95 * v + 0.05 * g * g
    step = m * lax.rsqrt(v + 1e-8) + 0.1 * w
    return (w - 0.02 * step).astype(BF), m, v


def solution(mesh):
    def step(x, dy, *arrays):
        (wg, wu, wd), m, v = (arrays[i : i + 3] for i in (0, 3, 6))
        N, D = x.shape[1:]
        FF = wg.shape[2]
        B, TB = 256, 256
        T, TN = FF // B, N // TB
        one = 2 * N * D * FF
        flat = lambda w: w.reshape(-1, w.shape[-1])
        wide, tokens = shape(N, FF), shape(N, D)
        whole = fixed((N, D))
        raw_whole = pl.BlockSpec((None, N, D), lambda t: (0, 0, 0), pipeline_mode=pl.Buffered(1))
        raw_rows = pl.BlockSpec((None, TB, D), lambda t: (0, t, 0))
        rows = down_by(TB, D)

        a1, wg1, wu1 = run("fetch_0", 1, TN, [x], [raw_rows], [tokens], [rows], norm, [Gather(0, wg, 0), Gather(1, wu, 0)], ["0", "0"], one)
        gate1, up1, hid1, wd1, wg2 = run(
            "glu_0", 2, T, [a1, flat(wg1), flat(wu1)], [whole, across(D, B), across(D, B)],
            [shape(N, FF, dtype=F32), shape(N, FF, dtype=F32), wide], [across(N, B)] * 3, glu,
            [Gather(0, wd, 0), Gather(1, wg, 1)], ["024579c"] * 2, 2 * one,
        )
        wd1, wg2 = flat(wd1), flat(wg2)
        h1, a2, wu2, wd2 = run(
            "lower_0", 3, TN, [hid1, wd1, x], [down_by(TB, FF), fixed((FF, D)), raw_rows],
            [tokens] * 2, [rows] * 2, lower, [Gather(0, wu, 1), Gather(1, wd, 1)], ["023457"] * 2, one,
        )
        wu2, wd2 = flat(wu2), flat(wd2)
        dg2, du2, gd2 = run(
            "both_1", 0, T, [a2, dy, wg2, wu2, wd2], [whole, raw_whole, across(D, B), across(D, B), down_by(B, D)],
            [wide, wide, shape(FF, D)], [across(N, B)] * 2 + [down_by(B, D)], both_ways, flops=4 * one, hold=[pltpu.VMEM((N, B), BF)],
        )
        gg2, gu2, fd2 = run(
            "grad_two_1", 4, T, [a2, dg2, du2], [whole, across(N, B), across(N, B)],
            [shape(D, FF)] * 2, [across(D, B)] * 2, grad_two, [SumA(gd2)], ["03388b"], 2 * one,
        )
        dh, fg2, sd2 = run(
            "grad_a_1", 5, TN, [dg2, du2, wg2, wu2, h1, dy], [down_by(TB, FF)] * 2 + [fixed((D, FF))] * 2 + [rows, raw_rows],
            [tokens], [rows], grad_a, [SumA(gg2), SumB(fd2)], ["022557", "01133446"], 2 * one,
        )
        dg1, du1, gd1, fu2, sg2 = run(
            "back_0", 6, T, [dh, wd1, gate1, up1, hid1], [whole, down_by(B, D)] + [across(N, B)] * 3,
            [wide, wide, shape(FF, D)], [across(N, B)] * 2 + [down_by(B, D)], back,
            [SumA(gu2), SumB(fg2)], ["022669b", "01133558"], 2 * one,
        )
        gg1, gu1, fd1, su2 = run(
            "grad_two_0", 7, T, [a1, dg1, du1], [whole, across(N, B), across(N, B)],
            [shape(D, FF)] * 2, [across(D, B)] * 2, grad_two, [SumA(gd1), SumB(fu2)], ["03388b", "0225577a"], 2 * one,
        )
        sg1, su1, sd1 = run("sum_last", 8, 1, [], [], [], [], None, [Sum(gg1), Sum(gu1), SumB(fd1)], flops=one)

        sums = [(sg1, sg2), (su1, su2), (sd1, sd2)]
        gradients = [jnp.stack(pair).astype(F32) for pair in sums]
        new = [adamw(w.astype(F32), mm, vv, g) for w, mm, vv, g in zip((wg, wu, wd), m, v, gradients, strict=True)]
        return tuple(one_[which] for which in range(3) for one_ in new)

    states, cut = P(("rep", "r", "s"), None, None), P(None, "s", None)
    return jax.shard_map(
        step,
        mesh=mesh,
        in_specs=(states, states) + (cut,) * 9,
        out_specs=(P("rep", "s", None),) * 9,
        check_vma=False,
    )
```
